32 devices in a mesh: coarse: 16 (over z, y, x), fine: 2 (over core).
Axes of the slice: x: 2, y: 2, z: 4, core: 2. Of those that a mesh axis runs over, the one named last changes fastest.
Arguments:
- fine_residual: bfloat16 [1024, 32, 128], P(('coarse', 'fine')), may hold values from -6 to 6
- prolong_blocks: bfloat16 [1024, 128, 128], P(('coarse', 'fine')), may hold values from -0.5 to 0.5
- aggregate_map: int32 [1024], P(('coarse', 'fine')), may hold values from 0 to 15, as said below
- block_counts: int32 [16], P('coarse'), may hold values from 8 to 16, as said below
- neighbors: int32 [256, 4], P('coarse'), may hold values from 0 to 47, as said below
- coarse_blocks: bfloat16 [256, 4, 128, 128], P('coarse'), may hold values from -0.29882812 to 0.29882812
- diag_values: float32 [256, 128], P('coarse'), may hold values from 2 to 16
Outputs:
- correction: float32 [1024, 32, 128], P(('coarse', 'fine'))
- coarse_solution: float32 [256, 32, 128], P('coarse')
The draws below stay inside these ranges and needn't reach their ends.
Inputs may be any that keep to these rules, and one draw needn't show every extreme that they name: `block_counts`: every owner has at least 8 live blocks (and at least 1); at least one owner has all 16 live. `aggregate_map`: A fine block names a live slot of its own owner: below block_counts of that owner. `neighbors`: column 0 names a live slot of the previous owner (0 to 15), columns 1 and 2 a slot of the same owner plus 16, column 3 a live slot of the next owner plus 2 * 16. Columns 1 and 2 may name dead slots.
All inputs are finite; a program needn't handle non-finite values.
Results may differ from the reference program's by a relative error of at most 0.0029.
Values may be sent and summed in bfloat16 or wider, within the bound.
No kernel may reach another device: no remote copies, remote signals or barrier semaphores. Data moves between devices by JAX's collectives and lax.ppermute only.
A program may use at most 64 MiB of HBM per device.

```python
import math
import jax
import jax.numpy as jnp
from jax import lax

BLK = 128
RHS = 32
NB = 4
STEPS = 6
CB = 16
OWNERS = 16
GROUP = 64
NFB = 1024
NCB = 256


def owner_counts(key):
    drawn_counts = jax.random.randint(jax.random.fold_in(key, 11), (OWNERS,), max(1, CB // 2), CB + 1)
    fullest = jax.random.randint(jax.random.fold_in(key, 13), (), 0, OWNERS)
    return jnp.where(jnp.arange(OWNERS) == fullest, CB, drawn_counts).astype(jnp.int32)


def draw_block_counts(key, part):
    return owner_counts(key)


def draw_aggregate_map(key, part):
    counts = owner_counts(key)
    raw_values = jax.random.randint(jax.random.fold_in(key, 17), (NFB,), 0, 1 << 20)
    owners = jnp.arange(NFB) // GROUP
    return (raw_values % counts[owners]).astype(jnp.int32)


def draw_neighbors(key, part):
    counts = owner_counts(key)
    owners = jnp.arange(NCB) // CB
    earlier_counts = counts[(owners - 1) % OWNERS]
    later_counts = counts[(owners + 1) % OWNERS]
    raw_before = jax.random.randint(jax.random.fold_in(key, 19), (NCB,), 0, 1 << 20)
    raw_after = jax.random.randint(jax.random.fold_in(key, 29), (NCB,), 0, 1 << 20)
    before = (raw_before % earlier_counts)[:, None]
    inside = jax.random.randint(jax.random.fold_in(key, 23), (NCB, 2), CB, 2 * CB)
    following = (2 * CB + raw_after % later_counts)[:, None]
    return jnp.concatenate([before, inside, following], axis=1).astype(jnp.int32)


def block_scale(rng, extent, cuts, smallest, top_value):
    def one(position, parts):
        draws = jax.random.uniform(jax.random.fold_in(jax.random.fold_in(rng, 6), position), (parts,), jnp.float32, smallest / len(cuts), top_value / len(cuts))
        return jnp.repeat(jnp.exp(draws), extent[position] // parts).reshape((-1,) + (1,) * (len(extent) - position - 1))

    level = one(*cuts[0])
    for cut in cuts[1:]:
        level = level * one(*cut)
    return level


def centred(rng, dims, width, reach, cuts=(), kind=jnp.bfloat16):
    values = jax.random.normal(rng, dims, jnp.float32) * width
    if len(cuts) > 0:
        values = block_scale(rng, dims, cuts, -0.22, 0.18) * values
    return jnp.clip(values, min=-reach, max=reach).astype(kind)


def setup_inputs(seed: int = 0) -> dict:
    streams_of = jax.random.split(jax.random.key(seed), 8)
    fine_residual = centred(streams_of[0], (NFB, RHS, BLK), 1.0, 6.0, ((0, 32),))
    prolong_blocks = centred(streams_of[1], (NFB, BLK, BLK), BLK ** -0.5, 0.5, ((0, 32),))
    aggregate_map = draw_aggregate_map(jax.random.fold_in(streams_of[7], 71), 0)
    block_counts = draw_block_counts(jax.random.fold_in(streams_of[7], 71), 0)
    neighbors = draw_neighbors(jax.random.fold_in(streams_of[7], 71), 0)
    coarse_blocks = centred(streams_of[5], (NCB, NB, BLK, BLK), 0.05, 0.29882812, ((0, 16),))
    diag_values = jnp.clip(jnp.exp(math.log(16.0) - 2.0794415 * jax.random.uniform(streams_of[6], (NCB, BLK), jnp.float32) ** block_scale(streams_of[6], (NCB, BLK), ((0, 16),), -0.2, 0.2)), 2.0, 16.0)
    return dict(fine_residual=fine_residual, prolong_blocks=prolong_blocks, aggregate_map=aggregate_map, block_counts=block_counts, neighbors=neighbors, coarse_blocks=coarse_blocks, diag_values=diag_values)


cheb_low = 0.5
cheb_high = 20.0


def apply_operator(update, coarse_blocks, neighbors, diag_values, live_mask):
    rounded = update.astype(jnp.bfloat16)
    empty = jnp.zeros((CB, RHS, BLK), jnp.bfloat16)
    padded = jnp.concatenate([empty, rounded, empty], axis=0)
    starts = (jnp.arange(NCB, dtype=jnp.int32) // CB) * CB
    index_rows = (starts[:, None] + neighbors).astype(jnp.int32)
    gathered = padded[index_rows]
    coupled = jnp.einsum("bjrk,bjkm->brm", gathered.astype(jnp.float32), coarse_blocks.astype(jnp.float32), precision=lax.Precision.HIGHEST)
    return live_mask[:, None, None] * (diag_values[:, None, :] * update + coupled)


def restrict_owner(inputs):
    residual_part, prolong_part, aggregate_part = inputs
    block_terms = jnp.einsum("irk,imk->irm", residual_part.astype(jnp.float32), prolong_part.astype(jnp.float32), precision=lax.Precision.HIGHEST)
    member = (aggregate_part[None, :] == jnp.arange(CB, dtype=jnp.int32)[:, None]).astype(jnp.float32)
    return jnp.einsum("ci,irm->crm", member, block_terms, precision=lax.Precision.HIGHEST)


def prolong_owner(inputs):
    solution_part, prolong_part, aggregate_part = inputs
    chosen = solution_part[aggregate_part]
    return jnp.einsum("irk,ikm->irm", chosen.astype(jnp.float32), prolong_part.astype(jnp.float32), precision=lax.Precision.HIGHEST)


def reference(fine_residual, prolong_blocks, aggregate_map, block_counts, neighbors, coarse_blocks, diag_values):
    live_mask = (jnp.arange(CB, dtype=jnp.int32)[None, :] < block_counts[:, None]).astype(jnp.float32).reshape(NCB)
    residual_groups = fine_residual.reshape(OWNERS, GROUP, RHS, BLK)
    prolong_groups = prolong_blocks.reshape(OWNERS, GROUP, BLK, BLK)
    aggregate_groups = aggregate_map.reshape(OWNERS, GROUP)
    coarse_rhs = lax.map(restrict_owner, (residual_groups, prolong_groups, aggregate_groups)).reshape(NCB, RHS, BLK)
    middle = 0.5 * (cheb_high + cheb_low)
    radius = 0.5 * (cheb_high - cheb_low)
    sigma_ratio = middle / radius
    rho_prev = 1.0 / sigma_ratio
    remainder = coarse_rhs
    update = remainder / middle
    solution = update
    for sweep_index in range(STEPS - 1):
        remainder = remainder - apply_operator(update, coarse_blocks, neighbors, diag_values, live_mask)
        rho_next = 1.0 / (2.0 * sigma_ratio - rho_prev)
        update = rho_next * rho_prev * update + (2.0 * rho_next / radius) * remainder
        solution = solution + update
        rho_prev = rho_next
    rounded = solution.astype(jnp.bfloat16).reshape(OWNERS, CB, RHS, BLK)
    correction = lax.map(prolong_owner, (rounded, prolong_groups, aggregate_groups)).reshape(NFB, RHS, BLK)
    return correction, solution
```

```python
import functools
import jax
import jax.numpy as jnp
from jax import lax
from jax.experimental import pallas as pl
from jax.experimental.pallas import tpu as pltpu
from jax.sharding import PartitionSpec as P

STEPS = 6
cheb_low = 0.5
cheb_high = 20.0

VMEM = pltpu.VMEM
SMEM = pltpu.SMEM
HBM = pltpu.HBM


def in_vmem(x):
    return pltpu.with_memory_space_constraint(x, VMEM)


def in_hbm(x):
    return pltpu.with_memory_space_constraint(x, HBM)


def in_smem(x):
    return pltpu.with_memory_space_constraint(x, SMEM)


def vmem_spec():
    return pl.BlockSpec(memory_space=VMEM)


def smem_spec():
    return pl.BlockSpec(memory_space=SMEM)


def params(limit):
    return pltpu.CompilerParams(vmem_limit_bytes=limit)


MIB = 1 << 20


def chebyshev_coefficients():
    middle = 0.5 * (cheb_high + cheb_low)
    radius = 0.5 * (cheb_high - cheb_low)
    sigma = middle / radius
    rho = 1.0 / sigma
    pairs = []
    for _ in range(STEPS - 1):
        rho_next = 1.0 / (2.0 * sigma - rho)
        pairs.append((rho_next * rho, 2.0 * rho_next / radius))
        rho = rho_next
    return middle, pairs


def swap_pairs(parity, owners, fine):
    pairs = []
    paired = set()
    for low in range(parity, owners - 1, 2):
        paired |= {low, low + 1}
        for k in range(fine):
            here = low * fine + k
            there = (low + 1) * fine + fine - 1 - k
            pairs += [(here, there), (there, here)]
    for owner in range(owners):
        if owner not in paired:
            pairs += [(owner * fine + k, owner * fine + fine - 1 - k) for k in range(fine)]
    return pairs


def restrict_kernel(
    chunks, fine, agg_ref, mine_ref, res_hbm, pro_hbm, pro_ref, *rest
):
    outs = rest[:fine]
    res_ref, acc_ref, sems = rest[fine:]
    blocks = pro_hbm.shape[0]
    size = blocks // chunks
    share = acc_ref.shape[2]

    def copies(c):
        part = pl.ds(c * size, size)
        return (
            pltpu.make_async_copy(pro_hbm.at[part], pro_ref.at[part], sems.at[0, c]),
            pltpu.make_async_copy(res_hbm.at[part], res_ref.at[part], sems.at[1, c]),
        )

    for c in range(chunks):
        for copy in copies(c):
            copy.start()
    acc_ref[...] = jnp.zeros_like(acc_ref)
    for c in range(chunks):
        for copy in copies(c):
            copy.wait()
        for i in range(c * size, (c + 1) * size):
            term = lax.dot_general(
                res_ref[i],
                pro_ref[i],
                (((1,), (1,)), ((), ())),
                preferred_element_type=jnp.float32,
            )
            slot = agg_ref[i]
            for s in range(fine):
                acc_ref[s, slot] += term[s * share : (s + 1) * share]
    mine = mine_ref[0]
    for m in range(fine):
        outs[m][...] = acc_ref[mine ^ m]


def own_kernel(nb_ref, w_ref, q_ref, out_ref):
    slots = q_ref.shape[0]
    for b in range(slots):
        left = jnp.concatenate(
            [q_ref[nb_ref[b, 1] - slots], q_ref[nb_ref[b, 2] - slots]], axis=1
        )
        right = jnp.concatenate([w_ref[b, 1], w_ref[b, 2]], axis=0)
        out_ref[b] = jnp.dot(left, right, preferred_element_type=jnp.float32)


def step_kernel(
    keep, scale, last, info_ref, count_ref, nb_ref, w_ref, odd_ref, even_ref, own_ref, diag_ref,
    rem_ref, upd_ref, sol_ref, *outs
):
    slots = own_ref.shape[0]
    odd_col = info_ref[1]
    even_col = info_ref[2]
    odd_ok = info_ref[3]
    even_ok = info_ref[4]
    count = count_ref[0]
    for b in range(slots):
        odd = odd_ref[nb_ref[b, odd_col] % slots]
        even = even_ref[nb_ref[b, even_col] % slots]
        odd = jnp.where(odd_ok > 0, odd, jnp.zeros_like(odd))
        even = jnp.where(even_ok > 0, even, jnp.zeros_like(even))
        left = jnp.concatenate([odd, even], axis=1)
        right = jnp.concatenate([w_ref[b, odd_col], w_ref[b, even_col]], axis=0)
        coupled = own_ref[b] + jnp.dot(left, right, preferred_element_type=jnp.float32)
        upd = upd_ref[b]
        applied = diag_ref[b : b + 1, :] * upd + coupled
        rem = rem_ref[b] - jnp.where(b < count, applied, jnp.zeros_like(applied))
        new = keep * upd + scale * rem
        sol = sol_ref[b] + new
        if last:
            outs[0][b] = sol
        else:
            outs[0][b] = rem
            outs[1][b] = new
            outs[2][b] = sol
            outs[3][b] = new.astype(outs[3].dtype)


def prolong_kernel(chunks, fine, agg_ref, mine_ref, pro_ref, *rest):
    parts = rest[:fine]
    cor_hbm, sol_ref, rounded_ref, cor_ref, sems = rest[fine:]
    share = parts[0].shape[1]
    mine = mine_ref[0]
    for s in range(fine):
        for m in range(fine):
            @pl.when((mine ^ m) == s)
            def _():
                piece = parts[m][...]
                sol_ref[:, s * share : (s + 1) * share, :] = piece
                rounded_ref[:, s * share : (s + 1) * share, :] = piece.astype(rounded_ref.dtype)
    blocks = pro_ref.shape[0]
    size = blocks // chunks

    def copy(c):
        part = pl.ds(c * size, size)
        return pltpu.make_async_copy(cor_ref.at[part], cor_hbm.at[part], sems.at[c])

    for c in range(chunks):
        for i in range(c * size, (c + 1) * size):
            cor_ref[i] = jnp.dot(
                rounded_ref[agg_ref[i]], pro_ref[i], preferred_element_type=jnp.float32
            )
        copy(c).start()
    for c in range(chunks):
        copy(c).wait()


def body(
    owners,
    fine,
    fine_residual,
    prolong_blocks,
    aggregate_map,
    block_counts,
    neighbors,
    coarse_blocks,
    diag_values,
):
    slots, _, width, _ = coarse_blocks.shape
    blocks, rhs, _ = fine_residual.shape
    share = rhs // fine
    f32 = jnp.float32
    bf16 = jnp.bfloat16
    piece = (slots, share, width)
    middle, pairs = chebyshev_coefficients()
    chunks = 4

    owner = lax.axis_index("coarse")
    k = lax.axis_index("fine")
    is_odd = owner % 2
    mine = jnp.where(is_odd == 1, fine - 1 - k, k)
    odd_ok = jnp.where(is_odd == 1, owner + 1 < owners, owner > 0)
    even_ok = jnp.where(is_odd == 1, True, owner + 1 < owners)
    info = jnp.stack(
        [
            mine,
            jnp.where(is_odd == 1, 3, 0),
            jnp.where(is_odd == 1, 0, 3),
            odd_ok.astype(jnp.int32),
            even_ok.astype(jnp.int32),
        ]
    ).astype(jnp.int32)
    info = in_smem(info)
    agg = in_smem(aggregate_map)
    count = in_smem(block_counts)
    nb = in_smem(neighbors)
    weights = in_vmem(coarse_blocks)
    diag = in_vmem(diag_values)

    pro, *sums = pl.pallas_call(
        functools.partial(restrict_kernel, chunks, fine),
        out_shape=[VMEM(prolong_blocks.shape, bf16)] + [VMEM(piece, f32)] * fine,
        in_specs=[smem_spec(), smem_spec()] + [pl.BlockSpec(memory_space=HBM)] * 2,
        out_specs=[vmem_spec()] * (fine + 1),
        scratch_shapes=[
            VMEM(fine_residual.shape, bf16),
            VMEM((fine,) + piece, f32),
            pltpu.SemaphoreType.DMA((2, chunks)),
        ],
        compiler_params=params(8 * MIB),
        name="restrict",
    )(agg, info, in_hbm(fine_residual), in_hbm(prolong_blocks))

    coarse_rhs = sums[0]
    for m in range(1, fine):
        coarse_rhs = coarse_rhs + lax.ppermute(
            sums[m], "fine", [(a, a ^ m) for a in range(fine)]
        )
    rem = coarse_rhs
    upd = coarse_rhs / middle
    sol = upd
    q = upd.astype(bf16)
    odd_pairs = swap_pairs(1, owners, fine)
    even_pairs = swap_pairs(0, owners, fine)
    for t, (keep, scale) in enumerate(pairs):
        last = t == len(pairs) - 1
        odd = lax.ppermute(q, ("coarse", "fine"), odd_pairs)
        even = lax.ppermute(q, ("coarse", "fine"), even_pairs)
        own = pl.pallas_call(
            own_kernel,
            out_shape=VMEM(piece, f32),
            in_specs=[smem_spec(), vmem_spec(), vmem_spec()],
            out_specs=vmem_spec(),
            compiler_params=params(4 * MIB),
            name="own",
        )(nb, weights, in_vmem(q))
        shapes = [VMEM(piece, f32)] if last else [VMEM(piece, f32)] * 3 + [VMEM(piece, bf16)]
        result = pl.pallas_call(
            functools.partial(step_kernel, keep, scale, last),
            out_shape=shapes,
            in_specs=[smem_spec()] * 3 + [vmem_spec()] * 8,
            out_specs=[vmem_spec()] * len(shapes),
            compiler_params=params(4 * MIB),
            name="step",
        )(
            info, count, nb, weights, in_vmem(odd), in_vmem(even), in_vmem(own), diag,
            in_vmem(rem), in_vmem(upd), in_vmem(sol),
        )
        if last:
            sol = result[0]
        else:
            rem, upd, sol, q = result

    parts = [sol] + [
        lax.ppermute(sol, "fine", [(a, a ^ m) for a in range(fine)]) for m in range(1, fine)
    ]
    correction, solution = pl.pallas_call(
        functools.partial(prolong_kernel, chunks, fine),
        out_shape=[
            HBM(fine_residual.shape, f32),
            jax.ShapeDtypeStruct((slots, rhs, width), f32),
        ],
        in_specs=[smem_spec(), smem_spec(), vmem_spec()] + [vmem_spec()] * fine,
        out_specs=[pl.BlockSpec(memory_space=HBM), vmem_spec()],
        scratch_shapes=[
            VMEM((slots, rhs, width), bf16),
            VMEM(fine_residual.shape, f32),
            pltpu.SemaphoreType.DMA((chunks,)),
        ],
        compiler_params=params(8 * MIB),
        name="prolong",
    )(agg, info, in_vmem(pro), *[in_vmem(p) for p in parts])
    return correction, solution


def solution(mesh):
    placed = (
        P(("coarse", "fine"), None, None),
        P(("coarse", "fine"), None, None),
        P(("coarse", "fine")),
        P("coarse"),
        P("coarse", None),
        P("coarse", None, None, None),
        P("coarse", None),
    )
    return jax.shard_map(
        functools.partial(body, mesh.shape["coarse"], mesh.shape["fine"]),
        mesh=mesh,
        in_specs=placed,
        out_specs=(P(("coarse", "fine"), None, None), P("coarse", None, None)),
        check_vma=False,
    )
```

```python
import functools
import jax
import jax.numpy as jnp
from jax import lax
from jax.experimental import pallas as pl
from jax.experimental.pallas import tpu as pltpu
from jax.sharding import PartitionSpec as P

STEPS = 6
cheb_low = 0.5
cheb_high = 20.0

VMEM = pltpu.VMEM
SMEM = pltpu.SMEM
HBM = pltpu.HBM


def in_vmem(x):
    return pltpu.with_memory_space_constraint(x, VMEM)


def in_hbm(x):
    return pltpu.with_memory_space_constraint(x, HBM)


def in_smem(x):
    return pltpu.with_memory_space_constraint(x, SMEM)


def vmem_spec():
    return pl.BlockSpec(memory_space=VMEM)


def smem_spec():
    return pl.BlockSpec(memory_space=SMEM)


def params(limit):
    return pltpu.CompilerParams(vmem_limit_bytes=limit)


MIB = 1 << 20


def chebyshev_coefficients():
    middle = 0.5 * (cheb_high + cheb_low)
    radius = 0.5 * (cheb_high - cheb_low)
    sigma = middle / radius
    rho = 1.0 / sigma
    pairs = []
    for _ in range(STEPS - 1):
        rho_next = 1.0 / (2.0 * sigma - rho)
        pairs.append((rho_next * rho, 2.0 * rho_next / radius))
        rho = rho_next
    return middle, pairs


def swap_pairs(parity, owners, fine):
    pairs = []
    paired = set()
    for low in range(parity, owners - 1, 2):
        paired |= {low, low + 1}
        for k in range(fine):
            here = low * fine + k
            there = (low + 1) * fine + fine - 1 - k
            pairs += [(here, there), (there, here)]
    for owner in range(owners):
        if owner not in paired:
            pairs += [(owner * fine + k, owner * fine + fine - 1 - k) for k in range(fine)]
    return pairs


def table_layout(slots, blocks):
    flags = 4 * slots + blocks
    return dict(agg=4 * slots, mine=flags, odd_col=flags + 1, even_col=flags + 2,
                odd_ok=flags + 3, even_ok=flags + 4, size=flags + 5)


def restrict_kernel(
    chunks, owners, fine, agg_hbm, nb_hbm, res_hbm, pro_hbm, pro_ref, tab_ref, *rest
):
    outs = rest[:fine]
    agg_ref, nb_ref, res_ref, acc_ref, sems, small_sems = rest[fine:]
    blocks = pro_hbm.shape[0]
    size = blocks // chunks
    slots = acc_ref.shape[1]
    share = acc_ref.shape[2]
    where = table_layout(slots, blocks)

    def copies(c):
        part = pl.ds(c * size, size)
        return (
            pltpu.make_async_copy(pro_hbm.at[part], pro_ref.at[part], sems.at[0, c]),
            pltpu.make_async_copy(res_hbm.at[part], res_ref.at[part], sems.at[1, c]),
        )

    agg_copy = pltpu.make_async_copy(agg_hbm, agg_ref, small_sems.at[0])
    nb_copy = pltpu.make_async_copy(nb_hbm, nb_ref, small_sems.at[1])
    agg_copy.start()
    for c in range(chunks):
        for copy in copies(c):
            copy.start()
    nb_copy.start()

    owner = lax.axis_index("coarse")
    k = lax.axis_index("fine")
    is_odd = owner % 2 == 1
    has_next = owner + 1 < owners
    mine = jnp.where(is_odd, fine - 1 - k, k)
    odd_col = jnp.where(is_odd, 3, 0)
    even_col = jnp.where(is_odd, 0, 3)
    tab_ref[where["mine"]] = mine
    tab_ref[where["odd_col"]] = odd_col
    tab_ref[where["even_col"]] = even_col
    tab_ref[where["odd_ok"]] = jnp.where(is_odd, has_next, owner > 0).astype(jnp.int32)
    tab_ref[where["even_ok"]] = jnp.where(is_odd, True, has_next).astype(jnp.int32)

    acc_ref[...] = jnp.zeros_like(acc_ref)
    agg_copy.wait()
    for i in range(blocks):
        tab_ref[where["agg"] + i] = agg_ref[i]
    for c in range(chunks):
        for copy in copies(c):
            copy.wait()
        for i in range(c * size, (c + 1) * size):
            term = lax.dot_general(
                res_ref[i],
                pro_ref[i],
                (((1,), (1,)), ((), ())),
                preferred_element_type=jnp.float32,
            )
            slot = agg_ref[i]
            for s in range(fine):
                acc_ref[s, slot] += term[s * share : (s + 1) * share]
    for m in range(fine):
        outs[m][...] = acc_ref[mine ^ m]
    nb_copy.wait()
    odd_base = jnp.where(is_odd, 2 * slots, 0)
    even_base = jnp.where(is_odd, 0, 2 * slots)
    for b in range(slots):
        tab_ref[b] = nb_ref[1, b] - slots
        tab_ref[slots + b] = nb_ref[2, b] - slots
        tab_ref[2 * slots + b] = nb_ref[odd_col, b] - odd_base
        tab_ref[3 * slots + b] = nb_ref[even_col, b] - even_base


def own_kernel(tab_ref, w_ref, q_ref, out_ref):
    slots = q_ref.shape[0]
    for b in range(slots):
        left = jnp.concatenate([q_ref[tab_ref[b]], q_ref[tab_ref[slots + b]]], axis=1)
        right = jnp.concatenate([w_ref[b, 1], w_ref[b, 2]], axis=0)
        out_ref[b] = jnp.dot(left, right, preferred_element_type=jnp.float32)


def step_kernel(
    keep, scale, last, where, count_ref, tab_ref, w_ref, odd_ref, even_ref, own_ref, diag_ref,
    rem_ref, upd_ref, sol_ref, *outs
):
    slots = own_ref.shape[0]
    odd_col = tab_ref[where["odd_col"]]
    even_col = tab_ref[where["even_col"]]
    odd_ok = tab_ref[where["odd_ok"]]
    even_ok = tab_ref[where["even_ok"]]
    count = count_ref[0]
    for b in range(slots):
        odd = odd_ref[tab_ref[2 * slots + b]]
        even = even_ref[tab_ref[3 * slots + b]]
        odd = jnp.where(odd_ok > 0, odd, jnp.zeros_like(odd))
        even = jnp.where(even_ok > 0, even, jnp.zeros_like(even))
        left = jnp.concatenate([odd, even], axis=1)
        right = jnp.concatenate([w_ref[b, odd_col], w_ref[b, even_col]], axis=0)
        coupled = own_ref[b] + jnp.dot(left, right, preferred_element_type=jnp.float32)
        upd = upd_ref[b]
        applied = diag_ref[b : b + 1, :] * upd + coupled
        rem = rem_ref[b] - jnp.where(b < count, applied, jnp.zeros_like(applied))
        new = keep * upd + scale * rem
        sol = sol_ref[b] + new
        if last:
            outs[0][b] = sol
        else:
            outs[0][b] = rem
            outs[1][b] = new
            outs[2][b] = sol
            outs[3][b] = new.astype(outs[3].dtype)


def prolong_kernel(chunks, fine, where, tab_ref, pro_ref, *rest):
    parts = rest[:fine]
    cor_hbm, sol_hbm, sol_ref, rounded_ref, cor_ref, sems, sol_sem = rest[fine:]
    share = parts[0].shape[1]
    mine = tab_ref[where["mine"]]
    for s in range(fine):
        for m in range(fine):
            @pl.when((mine ^ m) == s)
            def _():
                piece = parts[m][...]
                sol_ref[:, s * share : (s + 1) * share, :] = piece
                rounded_ref[:, s * share : (s + 1) * share, :] = piece.astype(rounded_ref.dtype)
    sol_copy = pltpu.make_async_copy(sol_ref, sol_hbm, sol_sem)
    sol_copy.start()
    blocks = pro_ref.shape[0]
    size = blocks // chunks

    def copy(c):
        part = pl.ds(c * size, size)
        return pltpu.make_async_copy(cor_ref.at[part], cor_hbm.at[part], sems.at[c])

    for c in range(chunks):
        for i in range(c * size, (c + 1) * size):
            cor_ref[i] = jnp.dot(
                rounded_ref[tab_ref[where["agg"] + i]],
                pro_ref[i],
                preferred_element_type=jnp.float32,
            )
        copy(c).start()
    sol_copy.wait()
    for c in range(chunks):
        copy(c).wait()


def body(
    owners,
    fine,
    fine_residual,
    prolong_blocks,
    aggregate_map,
    block_counts,
    neighbors,
    coarse_blocks,
    diag_values,
):
    slots, _, width, _ = coarse_blocks.shape
    blocks, rhs, _ = fine_residual.shape
    share = rhs // fine
    f32 = jnp.float32
    bf16 = jnp.bfloat16
    piece = (slots, share, width)
    middle, pairs = chebyshev_coefficients()
    chunks = 4
    where = table_layout(slots, blocks)

    pro, tab, *sums = pl.pallas_call(
        functools.partial(restrict_kernel, chunks, owners, fine),
        out_shape=[VMEM(prolong_blocks.shape, bf16), SMEM((where["size"],), jnp.int32)]
        + [VMEM(piece, f32)] * fine,
        in_specs=[pl.BlockSpec(memory_space=HBM)] * 4,
        out_specs=[vmem_spec(), smem_spec()] + [vmem_spec()] * fine,
        scratch_shapes=[
            SMEM((blocks,), jnp.int32),
            SMEM((neighbors.shape[1], slots), jnp.int32),
            VMEM(fine_residual.shape, bf16),
            VMEM((fine,) + piece, f32),
            pltpu.SemaphoreType.DMA((2, chunks)),
            pltpu.SemaphoreType.DMA((2,)),
        ],
        compiler_params=params(8 * MIB),
        name="restrict",
    )(
        in_hbm(aggregate_map), in_hbm(neighbors.T),
        in_hbm(fine_residual), in_hbm(prolong_blocks),
    )
    tab = in_smem(tab)
    coarse_blocks, diag_values, sums[0] = lax.optimization_barrier(
        (coarse_blocks, diag_values, sums[0])
    )
    weights = in_vmem(coarse_blocks)
    diag = in_vmem(diag_values)

    coarse_rhs = sums[0]
    for m in range(1, fine):
        coarse_rhs = coarse_rhs + lax.ppermute(
            sums[m], "fine", [(a, a ^ m) for a in range(fine)]
        )
    rem = coarse_rhs
    upd = coarse_rhs / middle
    sol = upd
    q = upd.astype(bf16)
    odd_pairs = swap_pairs(1, owners, fine)
    even_pairs = swap_pairs(0, owners, fine)
    for t, (keep, scale) in enumerate(pairs):
        last = t == len(pairs) - 1
        odd = lax.ppermute(q, ("coarse", "fine"), odd_pairs)
        even = lax.ppermute(q, ("coarse", "fine"), even_pairs)
        own = pl.pallas_call(
            own_kernel,
            out_shape=VMEM(piece, f32),
            in_specs=[smem_spec(), vmem_spec(), vmem_spec()],
            out_specs=vmem_spec(),
            compiler_params=params(4 * MIB),
            name="own",
        )(tab, weights, in_vmem(q))
        shapes = [VMEM(piece, f32)] if last else [VMEM(piece, f32)] * 3 + [VMEM(piece, bf16)]
        result = pl.pallas_call(
            functools.partial(step_kernel, keep, scale, last, where),
            out_shape=shapes,
            in_specs=[smem_spec()] * 2 + [vmem_spec()] * 8,
            out_specs=[vmem_spec()] * len(shapes),
            compiler_params=params(4 * MIB),
            name="step",
        )(
            block_counts, tab, weights, in_vmem(odd), in_vmem(even), in_vmem(own), diag,
            in_vmem(rem), in_vmem(upd), in_vmem(sol),
        )
        if last:
            sol = result[0]
        else:
            rem, upd, sol, q = result

    parts = [sol] + [
        lax.ppermute(sol, "fine", [(a, a ^ m) for a in range(fine)]) for m in range(1, fine)
    ]
    correction, solution = pl.pallas_call(
        functools.partial(prolong_kernel, chunks, fine, where),
        out_shape=[
            HBM(fine_residual.shape, f32),
            HBM((slots, rhs, width), f32),
        ],
        in_specs=[smem_spec(), vmem_spec()] + [vmem_spec()] * fine,
        out_specs=[pl.BlockSpec(memory_space=HBM)] * 2,
        scratch_shapes=[
            VMEM((slots, rhs, width), f32),
            VMEM((slots, rhs, width), bf16),
            VMEM(fine_residual.shape, f32),
            pltpu.SemaphoreType.DMA((chunks,)),
            pltpu.SemaphoreType.DMA,
        ],
        compiler_params=params(8 * MIB),
        name="prolong",
    )(tab, in_vmem(pro), *[in_vmem(p) for p in parts])
    return correction, solution


def solution(mesh):
    placed = (
        P(("coarse", "fine"), None, None),
        P(("coarse", "fine"), None, None),
        P(("coarse", "fine")),
        P("coarse"),
        P("coarse", None),
        P("coarse", None, None, None),
        P("coarse", None),
    )
    return jax.shard_map(
        functools.partial(body, mesh.shape["coarse"], mesh.shape["fine"]),
        mesh=mesh,
        in_specs=placed,
        out_specs=(P(("coarse", "fine"), None, None), P("coarse", None, None)),
        check_vma=False,
    )
```

```python
import functools
import jax
import jax.numpy as jnp
from jax import lax
from jax.experimental import pallas as pl
from jax.experimental.pallas import tpu as pltpu
from jax.sharding import PartitionSpec as P

STEPS = 6
cheb_low = 0.5
cheb_high = 20.0

VMEM = pltpu.VMEM
SMEM = pltpu.SMEM
HBM = pltpu.HBM


def in_vmem(x):
    return pltpu.with_memory_space_constraint(x, VMEM)


def in_hbm(x):
    return pltpu.with_memory_space_constraint(x, HBM)


def in_smem(x):
    return pltpu.with_memory_space_constraint(x, SMEM)


def vmem_spec():
    return pl.BlockSpec(memory_space=VMEM)


def smem_spec():
    return pl.BlockSpec(memory_space=SMEM)


def params(limit):
    return pltpu.CompilerParams(vmem_limit_bytes=limit)


MIB = 1 << 20


def chebyshev_coefficients():
    middle = 0.5 * (cheb_high + cheb_low)
    radius = 0.5 * (cheb_high - cheb_low)
    sigma = middle / radius
    rho = 1.0 / sigma
    pairs = []
    for _ in range(STEPS - 1):
        rho_next = 1.0 / (2.0 * sigma - rho)
        pairs.append((rho_next * rho, 2.0 * rho_next / radius))
        rho = rho_next
    return middle, pairs


def swap_pairs(parity, owners, fine):
    pairs = []
    paired = set()
    for low in range(parity, owners - 1, 2):
        paired |= {low, low + 1}
        for k in range(fine):
            here = low * fine + k
            there = (low + 1) * fine + fine - 1 - k
            pairs += [(here, there), (there, here)]
    for owner in range(owners):
        if owner not in paired:
            pairs += [(owner * fine + k, owner * fine + fine - 1 - k) for k in range(fine)]
    return pairs


def on_diagonal(rows):
    blank = jnp.zeros_like(rows[0])
    return jnp.concatenate(
        [
            jnp.concatenate([row if i == j else blank for j in range(len(rows))], axis=1)
            for i, row in enumerate(rows)
        ],
        axis=0,
    )


def table_layout(slots, blocks):
    flags = 4 * slots + blocks
    return dict(agg=4 * slots, mine=flags, odd_col=flags + 1, even_col=flags + 2,
                odd_ok=flags + 3, even_ok=flags + 4, size=flags + 5)


def restrict_kernel(
    chunks, owners, fine, agg_hbm, nb_hbm, res_hbm, pro_hbm, pro_ref, tab_ref, *rest
):
    outs = rest[:fine]
    agg_ref, nb_ref, res_ref, acc_ref, sems, small_sems = rest[fine:]
    blocks = pro_hbm.shape[0]
    size = blocks // chunks
    slots = acc_ref.shape[1]
    share = acc_ref.shape[2]
    where = table_layout(slots, blocks)

    def pro_copy(c):
        part = pl.ds(c * size, size)
        return pltpu.make_async_copy(pro_hbm.at[part], pro_ref.at[part], sems.at[c])

    res_copy = pltpu.make_async_copy(res_hbm, res_ref, small_sems.at[2])
    agg_copy = pltpu.make_async_copy(agg_hbm, agg_ref, small_sems.at[0])
    nb_copy = pltpu.make_async_copy(nb_hbm, nb_ref, small_sems.at[1])
    res_copy.start()
    for c in range(chunks):
        pro_copy(c).start()
    agg_copy.start()
    nb_copy.start()

    owner = lax.axis_index("coarse")
    k = lax.axis_index("fine")
    is_odd = owner % 2 == 1
    has_next = owner + 1 < owners
    mine = jnp.where(is_odd, fine - 1 - k, k)
    odd_col = jnp.where(is_odd, 3, 0)
    even_col = jnp.where(is_odd, 0, 3)
    odd_base = jnp.where(is_odd, 2 * slots, 0)
    even_base = jnp.where(is_odd, 0, 2 * slots)
    tab_ref[where["mine"]] = mine
    tab_ref[where["odd_col"]] = odd_col
    tab_ref[where["even_col"]] = even_col
    tab_ref[where["odd_ok"]] = jnp.where(is_odd, has_next, owner > 0).astype(jnp.int32)
    tab_ref[where["even_ok"]] = jnp.where(is_odd, True, has_next).astype(jnp.int32)

    acc_ref[...] = jnp.zeros_like(acc_ref)
    nb_copy.wait()
    for b in range(slots):
        tab_ref[b] = nb_ref[1, b] - slots
        tab_ref[slots + b] = nb_ref[2, b] - slots
        tab_ref[2 * slots + b] = nb_ref[odd_col, b] - odd_base
        tab_ref[3 * slots + b] = nb_ref[even_col, b] - even_base
    agg_copy.wait()
    for i in range(blocks):
        tab_ref[where["agg"] + i] = agg_ref[i]
    res_copy.wait()
    rhs = res_hbm.shape[1]
    group = 2 if size % 2 == 0 else 1
    for c in range(chunks):
        pro_copy(c).wait()
        for first in range(c * size, (c + 1) * size, group):
            members = range(first, first + group)
            terms = lax.dot_general(
                on_diagonal([res_ref[i] for i in members]),
                jnp.concatenate([pro_ref[i] for i in members], axis=1),
                (((1,), (1,)), ((), ())),
                preferred_element_type=jnp.float32,
            )
            for j, i in enumerate(members):
                slot = agg_ref[i]
                for s in range(fine):
                    top = j * rhs + s * share
                    acc_ref[s, slot] += terms[top : top + share]
    for m in range(fine):
        outs[m][...] = acc_ref[mine ^ m]


def mid_kernel(first, before, keep, scale, middle, where, count_ref, tab_ref, w_ref, q_ref,
               even_ref, diag_ref, *refs):
    state, outs = refs[: 1 if first else 4], refs[1 if first else 4 :]
    slots = q_ref.shape[0]
    even_col = tab_ref[where["even_col"]]
    even_ok = tab_ref[where["even_ok"]]
    count = count_ref[0]
    for b in range(slots):
        even = even_ref[tab_ref[3 * slots + b]]
        even = jnp.where(even_ok > 0, even, jnp.zeros_like(even))
        left = jnp.concatenate(
            [q_ref[tab_ref[b]], q_ref[tab_ref[slots + b]], even], axis=1
        )
        right = jnp.concatenate([w_ref[b, 1], w_ref[b, 2], w_ref[b, even_col]], axis=0)
        coupled = jnp.dot(left, right, preferred_element_type=jnp.float32)
        if first:
            rem = state[0][b]
            upd = rem / middle
            sol = upd
        else:
            late = state[3][b]
            rem = state[0][b] - late
            upd = state[1][b] - before * late
            sol = state[2][b] - before * late
        applied = diag_ref[b : b + 1, :] * upd + coupled
        rem = rem - jnp.where(b < count, applied, jnp.zeros_like(applied))
        base = keep * upd + scale * rem
        outs[0][b] = sol + base
        if len(outs) > 1:
            outs[1][b] = rem
            outs[2][b] = base


def step_kernel(scale, last, where, count_ref, tab_ref, w_ref, odd_ref, base_ref, *outs):
    slots, share, _ = odd_ref.shape
    odd_col = tab_ref[where["odd_col"]]
    live = jnp.where(tab_ref[where["odd_ok"]] > 0, count_ref[0], 0)
    group = 2 if slots % 2 == 0 else 1
    for first in range(0, slots, group):
        members = range(first, first + group)
        left = on_diagonal([odd_ref[tab_ref[2 * slots + b]] for b in members])
        right = jnp.concatenate([w_ref[b, odd_col] for b in members], axis=0)
        both = jnp.dot(left, right, preferred_element_type=jnp.float32)
        for i, b in enumerate(members):
            late = both[i * share : (i + 1) * share]
            late = jnp.where(b < live, late, jnp.zeros_like(late))
            new = base_ref[b] - scale * late
            if last:
                outs[0][b] = new
            else:
                outs[0][b] = late
                outs[1][b] = new.astype(outs[1].dtype)


def load_kernel(chunks, after_ref, w_hbm, diag_hbm, w_ref, diag_ref, sems, diag_sem):
    size = w_hbm.shape[0] // chunks
    copies = [
        pltpu.make_async_copy(
            w_hbm.at[pl.ds(c * size, size)], w_ref.at[pl.ds(c * size, size)], sems.at[c]
        )
        for c in range(chunks)
    ]
    copies.append(pltpu.make_async_copy(diag_hbm, diag_ref, diag_sem))
    for copy in copies:
        copy.start()
    for copy in copies:
        copy.wait()


def prolong_kernel(chunks, fine, where, tab_ref, pro_ref, *rest):
    parts = rest[:fine]
    cor_hbm, sol_hbm, sol_ref, rounded_ref, cor_ref, sems, sol_sem = rest[fine:]
    share = parts[0].shape[1]
    mine = tab_ref[where["mine"]]
    for s in range(fine):
        for m in range(fine):
            @pl.when((mine ^ m) == s)
            def _():
                piece = parts[m][...]
                sol_ref[:, s * share : (s + 1) * share, :] = piece
                rounded_ref[:, s * share : (s + 1) * share, :] = piece.astype(rounded_ref.dtype)
    sol_copy = pltpu.make_async_copy(sol_ref, sol_hbm, sol_sem)
    sol_copy.start()
    blocks = pro_ref.shape[0]
    size = blocks // chunks
    rhs = rounded_ref.shape[1]
    group = 2 if size % 2 == 0 else 1

    def copy(c):
        part = pl.ds(c * size, size)
        return pltpu.make_async_copy(cor_ref.at[part], cor_hbm.at[part], sems.at[c])

    for c in range(chunks):
        for first in range(c * size, (c + 1) * size, group):
            members = range(first, first + group)
            both = jnp.dot(
                on_diagonal([rounded_ref[tab_ref[where["agg"] + i]] for i in members]),
                jnp.concatenate([pro_ref[i] for i in members], axis=0),
                preferred_element_type=jnp.float32,
            )
            for j, i in enumerate(members):
                cor_ref[i] = both[j * rhs : (j + 1) * rhs]
        copy(c).start()
    sol_copy.wait()
    for c in range(chunks):
        copy(c).wait()


def body(
    owners,
    fine,
    fine_residual,
    prolong_blocks,
    aggregate_map,
    block_counts,
    neighbors,
    coarse_blocks,
    diag_values,
):
    slots, _, width, _ = coarse_blocks.shape
    blocks, rhs, _ = fine_residual.shape
    share = rhs // fine
    f32 = jnp.float32
    bf16 = jnp.bfloat16
    piece = (slots, share, width)
    middle, pairs = chebyshev_coefficients()
    chunks = 2
    where = table_layout(slots, blocks)

    pro, tab, *sums = pl.pallas_call(
        functools.partial(restrict_kernel, chunks, owners, fine),
        out_shape=[VMEM(prolong_blocks.shape, bf16), SMEM((where["size"],), jnp.int32)]
        + [VMEM(piece, f32)] * fine,
        in_specs=[pl.BlockSpec(memory_space=HBM)] * 4,
        out_specs=[vmem_spec(), smem_spec()] + [vmem_spec()] * fine,
        scratch_shapes=[
            SMEM((blocks,), jnp.int32),
            SMEM((neighbors.shape[1], slots), jnp.int32),
            VMEM(fine_residual.shape, bf16),
            VMEM((fine,) + piece, f32),
            pltpu.SemaphoreType.DMA((chunks,)),
            pltpu.SemaphoreType.DMA((3,)),
        ],
        compiler_params=params(8 * MIB),
        name="restrict",
    )(
        in_hbm(aggregate_map), in_hbm(neighbors.T),
        in_hbm(fine_residual), in_hbm(prolong_blocks),
    )
    tab = in_smem(tab)
    coarse_rhs = sums[0]
    for m in range(1, fine):
        coarse_rhs = coarse_rhs + lax.ppermute(
            sums[m], "fine", [(a, a ^ m) for a in range(fine)]
        )
    state = [coarse_rhs]
    q = (coarse_rhs / middle).astype(bf16)
    before = 0.0
    odd_pairs = swap_pairs(1, owners, fine)
    even_pairs = swap_pairs(0, owners, fine)
    for t, (keep, scale) in enumerate(pairs):
        last = t == len(pairs) - 1
        odd = lax.ppermute(q, ("coarse", "fine"), odd_pairs)
        even = lax.ppermute(q, ("coarse", "fine"), even_pairs)
        if t == 0:
            weights, diag = pl.pallas_call(
                functools.partial(load_kernel, chunks),
                out_shape=[VMEM(coarse_blocks.shape, bf16), VMEM(diag_values.shape, f32)],
                in_specs=[vmem_spec()] + [pl.BlockSpec(memory_space=HBM)] * 2,
                out_specs=[vmem_spec()] * 2,
                scratch_shapes=[pltpu.SemaphoreType.DMA((chunks,)), pltpu.SemaphoreType.DMA],
                compiler_params=params(2 * MIB),
                name="load",
            )(in_vmem(q), in_hbm(coarse_blocks), in_hbm(diag_values))
            weights = in_vmem(weights)
            diag = in_vmem(diag)
        kept = 1 if last else 3
        total, *carry = pl.pallas_call(
            functools.partial(mid_kernel, t == 0, before, keep, scale, middle, where),
            out_shape=[VMEM(piece, f32)] * kept,
            in_specs=[smem_spec()] * 2 + [vmem_spec()] * (4 + len(state)),
            out_specs=[vmem_spec()] * kept,
            compiler_params=params(4 * MIB),
            name="mid",
        )(
            block_counts, tab, weights, in_vmem(q), in_vmem(even), diag,
            *[in_vmem(x) for x in state],
        )
        shapes = [VMEM(piece, f32)] if last else [VMEM(piece, f32), VMEM(piece, bf16)]
        result = pl.pallas_call(
            functools.partial(step_kernel, scale, last, where),
            out_shape=shapes,
            in_specs=[smem_spec()] * 2 + [vmem_spec()] * 3,
            out_specs=[vmem_spec()] * len(shapes),
            compiler_params=params(4 * MIB),
            name="step",
        )(block_counts, tab, weights, in_vmem(odd), in_vmem(total if last else carry[1]))
        if last:
            sol = result[0]
        else:
            late, q = result
            state = [carry[0], carry[1], total, late]
            before = scale

    parts = [sol] + [
        lax.ppermute(sol, "fine", [(a, a ^ m) for a in range(fine)]) for m in range(1, fine)
    ]
    correction, solution = pl.pallas_call(
        functools.partial(prolong_kernel, chunks, fine, where),
        out_shape=[
            HBM(fine_residual.shape, f32),
            HBM((slots, rhs, width), f32),
        ],
        in_specs=[smem_spec(), vmem_spec()] + [vmem_spec()] * fine,
        out_specs=[pl.BlockSpec(memory_space=HBM)] * 2,
        scratch_shapes=[
            VMEM((slots, rhs, width), f32),
            VMEM((slots, rhs, width), bf16),
            VMEM(fine_residual.shape, f32),
            pltpu.SemaphoreType.DMA((chunks,)),
            pltpu.SemaphoreType.DMA,
        ],
        compiler_params=params(8 * MIB),
        name="prolong",
    )(tab, in_vmem(pro), *[in_vmem(p) for p in parts])
    return correction, solution


def solution(mesh):
    placed = (
        P(("coarse", "fine"), None, None),
        P(("coarse", "fine"), None, None),
        P(("coarse", "fine")),
        P("coarse"),
        P("coarse", None),
        P("coarse", None, None, None),
        P("coarse", None),
    )
    return jax.shard_map(
        functools.partial(body, mesh.shape["coarse"], mesh.shape["fine"]),
        mesh=mesh,
        in_specs=placed,
        out_specs=(P(("coarse", "fine"), None, None), P("coarse", None, None)),
        check_vma=False,
    )
```

```python
import functools
import jax
import jax.numpy as jnp
from jax import lax
from jax.experimental import pallas as pl
from jax.experimental.pallas import tpu as pltpu
from jax.sharding import PartitionSpec as P

STEPS = 6
cheb_low = 0.5
cheb_high = 20.0

VMEM = pltpu.VMEM
SMEM = pltpu.SMEM
HBM = pltpu.HBM


def in_vmem(x):
    return pltpu.with_memory_space_constraint(x, VMEM)


def in_hbm(x):
    return pltpu.with_memory_space_constraint(x, HBM)


def in_smem(x):
    return pltpu.with_memory_space_constraint(x, SMEM)


def vmem_spec():
    return pl.BlockSpec(memory_space=VMEM)


def smem_spec():
    return pl.BlockSpec(memory_space=SMEM)


def params(limit):
    return pltpu.CompilerParams(vmem_limit_bytes=limit)


MIB = 1 << 20


def chebyshev_coefficients():
    middle = 0.5 * (cheb_high + cheb_low)
    radius = 0.5 * (cheb_high - cheb_low)
    sigma = middle / radius
    rho = 1.0 / sigma
    pairs = []
    for _ in range(STEPS - 1):
        rho_next = 1.0 / (2.0 * sigma - rho)
        pairs.append((rho_next * rho, 2.0 * rho_next / radius))
        rho = rho_next
    return middle, pairs


def swap_pairs(parity, owners, fine):
    pairs = []
    paired = set()
    for low in range(parity, owners - 1, 2):
        paired |= {low, low + 1}
        for k in range(fine):
            here = low * fine + k
            there = (low + 1) * fine + fine - 1 - k
            pairs += [(here, there), (there, here)]
    for owner in range(owners):
        if owner not in paired:
            pairs += [(owner * fine + k, owner * fine + fine - 1 - k) for k in range(fine)]
    return pairs


def on_diagonal(rows):
    blank = jnp.zeros_like(rows[0])
    return jnp.concatenate(
        [
            jnp.concatenate([row if i == j else blank for j in range(len(rows))], axis=1)
            for i, row in enumerate(rows)
        ],
        axis=0,
    )


def table_layout(slots, blocks):
    flags = 4 * slots + blocks
    return dict(agg=4 * slots, mine=flags, odd_col=flags + 1, even_col=flags + 2,
                odd_ok=flags + 3, even_ok=flags + 4, size=flags + 5)


def restrict_kernel(
    chunks, owners, fine, agg_hbm, nb_hbm, res_hbm, pro_hbm, pro_ref, tab_ref, *rest
):
    outs = rest[:fine]
    agg_ref, nb_ref, res_ref, acc_ref, sems, small_sems = rest[fine:]
    blocks = pro_hbm.shape[0]
    size = blocks // chunks
    slots = acc_ref.shape[1]
    share = acc_ref.shape[2]
    where = table_layout(slots, blocks)

    def pro_copy(c):
        part = pl.ds(c * size, size)
        return pltpu.make_async_copy(pro_hbm.at[part], pro_ref.at[part], sems.at[c])

    res_copy = pltpu.make_async_copy(res_hbm, res_ref, small_sems.at[2])
    agg_copy = pltpu.make_async_copy(agg_hbm, agg_ref, small_sems.at[0])
    nb_copy = pltpu.make_async_copy(nb_hbm, nb_ref, small_sems.at[1])
    res_copy.start()
    for c in range(chunks):
        pro_copy(c).start()
    agg_copy.start()
    nb_copy.start()

    owner = lax.axis_index("coarse")
    k = lax.axis_index("fine")
    is_odd = owner % 2 == 1
    has_next = owner + 1 < owners
    mine = jnp.where(is_odd, fine - 1 - k, k)
    odd_col = jnp.where(is_odd, 3, 0)
    even_col = jnp.where(is_odd, 0, 3)
    odd_base = jnp.where(is_odd, 2 * slots, 0)
    even_base = jnp.where(is_odd, 0, 2 * slots)
    tab_ref[where["mine"]] = mine
    tab_ref[where["odd_col"]] = odd_col
    tab_ref[where["even_col"]] = even_col
    tab_ref[where["odd_ok"]] = jnp.where(is_odd, has_next, owner > 0).astype(jnp.int32)
    tab_ref[where["even_ok"]] = jnp.where(is_odd, True, has_next).astype(jnp.int32)

    acc_ref[...] = jnp.zeros_like(acc_ref)
    nb_copy.wait()
    for b in range(slots):
        tab_ref[b] = nb_ref[1, b] - slots
        tab_ref[slots + b] = nb_ref[2, b] - slots
        tab_ref[2 * slots + b] = nb_ref[odd_col, b] - odd_base
        tab_ref[3 * slots + b] = nb_ref[even_col, b] - even_base
    agg_copy.wait()
    for i in range(blocks):
        tab_ref[where["agg"] + i] = agg_ref[i]
    res_copy.wait()
    rhs = res_hbm.shape[1]
    group = 2 if size % 2 == 0 else 1
    for c in range(chunks):
        pro_copy(c).wait()
        for first in range(c * size, (c + 1) * size, group):
            members = range(first, first + group)
            terms = lax.dot_general(
                on_diagonal([res_ref[i] for i in members]),
                jnp.concatenate([pro_ref[i] for i in members], axis=1),
                (((1,), (1,)), ((), ())),
                preferred_element_type=jnp.float32,
            )
            for j, i in enumerate(members):
                slot = agg_ref[i]
                for s in range(fine):
                    top = j * rhs + s * share
                    acc_ref[s, slot] += terms[top : top + share]
    for m in range(fine):
        outs[m][...] = acc_ref[mine ^ m]


def mid_kernel(first, before, keep, scale, middle, where, count_ref, tab_ref, w_ref, q_ref,
               even_ref, diag_ref, *refs):
    state, outs = refs[: 1 if first else 4], refs[1 if first else 4 :]
    slots = q_ref.shape[0]
    even_col = tab_ref[where["even_col"]]
    even_ok = tab_ref[where["even_ok"]]
    count = count_ref[0]
    for b in range(slots):
        even = even_ref[tab_ref[3 * slots + b]]
        even = jnp.where(even_ok > 0, even, jnp.zeros_like(even))
        left = jnp.concatenate(
            [q_ref[tab_ref[b]], q_ref[tab_ref[slots + b]], even], axis=1
        )
        right = jnp.concatenate([w_ref[b, 1], w_ref[b, 2], w_ref[b, even_col]], axis=0)
        coupled = jnp.dot(left, right, preferred_element_type=jnp.float32)
        if first:
            rem = state[0][b]
            upd = rem / middle
            sol = upd
        else:
            late = state[3][b]
            rem = state[0][b] - late
            upd = state[1][b] - before * late
            sol = state[2][b] - before * late
        applied = diag_ref[b : b + 1, :] * upd + coupled
        rem = rem - jnp.where(b < count, applied, jnp.zeros_like(applied))
        base = keep * upd + scale * rem
        outs[0][b] = sol + base
        if len(outs) > 1:
            outs[1][b] = rem
            outs[2][b] = base


def step_kernel(scale, last, where, count_ref, tab_ref, w_ref, odd_ref, base_ref, *outs):
    slots, share, _ = odd_ref.shape
    odd_col = tab_ref[where["odd_col"]]
    live = jnp.where(tab_ref[where["odd_ok"]] > 0, count_ref[0], 0)
    group = 2 if slots % 2 == 0 else 1
    for first in range(0, slots, group):
        members = range(first, first + group)
        left = on_diagonal([odd_ref[tab_ref[2 * slots + b]] for b in members])
        right = jnp.concatenate([w_ref[b, odd_col] for b in members], axis=0)
        both = jnp.dot(left, right, preferred_element_type=jnp.float32)
        for i, b in enumerate(members):
            late = both[i * share : (i + 1) * share]
            late = jnp.where(b < live, late, jnp.zeros_like(late))
            new = base_ref[b] - scale * late
            if last:
                outs[0][b] = new
            else:
                outs[0][b] = late
                outs[1][b] = new.astype(outs[1].dtype)


def share_kernel(m, chunks, where, tab_ref, pro_ref, part_ref, *rest):
    cor_hbm, sol_hbm, rounded_ref, cor_ref, sems, sol_sem = rest[-6:]
    share = part_ref.shape[1]
    rows = pl.ds(pl.multiple_of((tab_ref[where["mine"]] ^ m) * share, share), share)
    sol_copy = pltpu.make_async_copy(part_ref, sol_hbm.at[:, rows], sol_sem)
    sol_copy.start()
    rounded_ref[...] = part_ref[...].astype(rounded_ref.dtype)
    blocks = pro_ref.shape[0]
    size = blocks // chunks
    group = 2 if size % 2 == 0 else 1

    def copy(c):
        part = pl.ds(c * size, size)
        return pltpu.make_async_copy(cor_ref.at[part], cor_hbm.at[part, rows], sems.at[c])

    for c in range(chunks):
        for first in range(c * size, (c + 1) * size, group):
            members = range(first, first + group)
            both = jnp.dot(
                on_diagonal([rounded_ref[tab_ref[where["agg"] + i]] for i in members]),
                jnp.concatenate([pro_ref[i] for i in members], axis=0),
                preferred_element_type=jnp.float32,
            )
            for j, i in enumerate(members):
                cor_ref[i] = both[j * share : (j + 1) * share]
        copy(c).start()
    sol_copy.wait()
    for c in range(chunks):
        copy(c).wait()


def load_kernel(chunks, after_ref, w_hbm, diag_hbm, w_ref, diag_ref, sems, diag_sem):
    size = w_hbm.shape[0] // chunks
    copies = [
        pltpu.make_async_copy(
            w_hbm.at[pl.ds(c * size, size)], w_ref.at[pl.ds(c * size, size)], sems.at[c]
        )
        for c in range(chunks)
    ]
    copies.append(pltpu.make_async_copy(diag_hbm, diag_ref, diag_sem))
    for copy in copies:
        copy.start()
    for copy in copies:
        copy.wait()


def prolong_kernel(chunks, fine, where, tab_ref, pro_ref, *rest):
    parts = rest[:fine]
    cor_hbm, sol_hbm, sol_ref, rounded_ref, cor_ref, sems, sol_sem = rest[fine:]
    share = parts[0].shape[1]
    mine = tab_ref[where["mine"]]
    for s in range(fine):
        for m in range(fine):
            @pl.when((mine ^ m) == s)
            def _():
                piece = parts[m][...]
                sol_ref[:, s * share : (s + 1) * share, :] = piece
                rounded_ref[:, s * share : (s + 1) * share, :] = piece.astype(rounded_ref.dtype)
    sol_copy = pltpu.make_async_copy(sol_ref, sol_hbm, sol_sem)
    sol_copy.start()
    blocks = pro_ref.shape[0]
    size = blocks // chunks
    rhs = rounded_ref.shape[1]
    group = 2 if size % 2 == 0 else 1

    def copy(c):
        part = pl.ds(c * size, size)
        return pltpu.make_async_copy(cor_ref.at[part], cor_hbm.at[part], sems.at[c])

    for c in range(chunks):
        for first in range(c * size, (c + 1) * size, group):
            members = range(first, first + group)
            both = jnp.dot(
                on_diagonal([rounded_ref[tab_ref[where["agg"] + i]] for i in members]),
                jnp.concatenate([pro_ref[i] for i in members], axis=0),
                preferred_element_type=jnp.float32,
            )
            for j, i in enumerate(members):
                cor_ref[i] = both[j * rhs : (j + 1) * rhs]
        copy(c).start()
    sol_copy.wait()
    for c in range(chunks):
        copy(c).wait()


def body(
    owners,
    fine,
    fine_residual,
    prolong_blocks,
    aggregate_map,
    block_counts,
    neighbors,
    coarse_blocks,
    diag_values,
):
    slots, _, width, _ = coarse_blocks.shape
    blocks, rhs, _ = fine_residual.shape
    share = rhs // fine
    f32 = jnp.float32
    bf16 = jnp.bfloat16
    piece = (slots, share, width)
    middle, pairs = chebyshev_coefficients()
    chunks = 2
    where = table_layout(slots, blocks)

    pro, tab, *sums = pl.pallas_call(
        functools.partial(restrict_kernel, chunks, owners, fine),
        out_shape=[VMEM(prolong_blocks.shape, bf16), SMEM((where["size"],), jnp.int32)]
        + [VMEM(piece, f32)] * fine,
        in_specs=[pl.BlockSpec(memory_space=HBM)] * 4,
        out_specs=[vmem_spec(), smem_spec()] + [vmem_spec()] * fine,
        scratch_shapes=[
            SMEM((blocks,), jnp.int32),
            SMEM((neighbors.shape[1], slots), jnp.int32),
            VMEM(fine_residual.shape, bf16),
            VMEM((fine,) + piece, f32),
            pltpu.SemaphoreType.DMA((chunks,)),
            pltpu.SemaphoreType.DMA((3,)),
        ],
        compiler_params=params(8 * MIB),
        name="restrict",
    )(
        in_hbm(aggregate_map), in_hbm(neighbors.T),
        in_hbm(fine_residual), in_hbm(prolong_blocks),
    )
    tab = in_smem(tab)
    coarse_rhs = sums[0]
    for m in range(1, fine):
        coarse_rhs = coarse_rhs + lax.ppermute(
            sums[m], "fine", [(a, a ^ m) for a in range(fine)]
        )
    state = [coarse_rhs]
    q = (coarse_rhs / middle).astype(bf16)
    before = 0.0
    odd_pairs = swap_pairs(1, owners, fine)
    even_pairs = swap_pairs(0, owners, fine)
    for t, (keep, scale) in enumerate(pairs):
        last = t == len(pairs) - 1
        odd = lax.ppermute(q, ("coarse", "fine"), odd_pairs)
        even = lax.ppermute(q, ("coarse", "fine"), even_pairs)
        if t == 0:
            weights, diag = pl.pallas_call(
                functools.partial(load_kernel, chunks),
                out_shape=[VMEM(coarse_blocks.shape, bf16), VMEM(diag_values.shape, f32)],
                in_specs=[vmem_spec()] + [pl.BlockSpec(memory_space=HBM)] * 2,
                out_specs=[vmem_spec()] * 2,
                scratch_shapes=[pltpu.SemaphoreType.DMA((chunks,)), pltpu.SemaphoreType.DMA],
                compiler_params=params(2 * MIB),
                name="load",
            )(in_vmem(q), in_hbm(coarse_blocks), in_hbm(diag_values))
            weights = in_vmem(weights)
            diag = in_vmem(diag)
        kept = 1 if last else 3
        total, *carry = pl.pallas_call(
            functools.partial(mid_kernel, t == 0, before, keep, scale, middle, where),
            out_shape=[VMEM(piece, f32)] * kept,
            in_specs=[smem_spec()] * 2 + [vmem_spec()] * (4 + len(state)),
            out_specs=[vmem_spec()] * kept,
            compiler_params=params(4 * MIB),
            name="mid",
        )(
            block_counts, tab, weights, in_vmem(q), in_vmem(even), diag,
            *[in_vmem(x) for x in state],
        )
        shapes = [VMEM(piece, f32)] if last else [VMEM(piece, f32), VMEM(piece, bf16)]
        result = pl.pallas_call(
            functools.partial(step_kernel, scale, last, where),
            out_shape=shapes,
            in_specs=[smem_spec()] * 2 + [vmem_spec()] * 3,
            out_specs=[vmem_spec()] * len(shapes),
            compiler_params=params(4 * MIB),
            name="step",
        )(block_counts, tab, weights, in_vmem(odd), in_vmem(total if last else carry[1]))
        if last:
            sol = result[0]
        else:
            late, q = result
            state = [carry[0], carry[1], total, late]
            before = scale

    parts = [sol] + [
        lax.ppermute(sol, "fine", [(a, a ^ m) for a in range(fine)]) for m in range(1, fine)
    ]
    if share % 8 == 0:
        buffers = []
        for m in range(fine):
            buffers = pl.pallas_call(
                functools.partial(share_kernel, m, chunks, where),
                out_shape=[
                    HBM(fine_residual.shape, f32),
                    HBM((slots, rhs, width), f32),
                ],
                in_specs=[smem_spec(), vmem_spec(), vmem_spec()]
                + [pl.BlockSpec(memory_space=HBM)] * len(buffers),
                out_specs=[pl.BlockSpec(memory_space=HBM)] * 2,
                scratch_shapes=[
                    VMEM(piece, bf16),
                    VMEM((blocks, share, width), f32),
                    pltpu.SemaphoreType.DMA((chunks,)),
                    pltpu.SemaphoreType.DMA,
                ],
                input_output_aliases={3 + i: i for i in range(len(buffers))},
                compiler_params=params(8 * MIB),
                name="prolong",
            )(tab, in_vmem(pro), in_vmem(parts[m]), *[in_hbm(x) for x in buffers])
        correction, solution = buffers
    else:
        correction, solution = pl.pallas_call(
            functools.partial(prolong_kernel, chunks, fine, where),
            out_shape=[
                HBM(fine_residual.shape, f32),
                HBM((slots, rhs, width), f32),
            ],
            in_specs=[smem_spec(), vmem_spec()] + [vmem_spec()] * fine,
            out_specs=[pl.BlockSpec(memory_space=HBM)] * 2,
            scratch_shapes=[
                VMEM((slots, rhs, width), f32),
                VMEM((slots, rhs, width), bf16),
                VMEM(fine_residual.shape, f32),
                pltpu.SemaphoreType.DMA((chunks,)),
                pltpu.SemaphoreType.DMA,
            ],
            compiler_params=params(8 * MIB),
            name="prolong",
        )(tab, in_vmem(pro), *[in_vmem(p) for p in parts])
    return correction, solution


def solution(mesh):
    placed = (
        P(("coarse", "fine"), None, None),
        P(("coarse", "fine"), None, None),
        P(("coarse", "fine")),
        P("coarse"),
        P("coarse", None),
        P("coarse", None, None, None),
        P("coarse", None),
    )
    return jax.shard_map(
        functools.partial(body, mesh.shape["coarse"], mesh.shape["fine"]),
        mesh=mesh,
        in_specs=placed,
        out_specs=(P(("coarse", "fine"), None, None), P("coarse", None, None)),
        check_vma=False,
    )
```
